32 devices in a mesh: dev: 32 (over z, y, x, core).
Axes of the slice: x: 2, y: 2, z: 4, core: 2. Of those that a mesh axis runs over, the one named last changes fastest.
Arguments:
- upstream: bfloat16 [16384, 1024], P('dev'), may hold values from -6 to 6
- bag: int32 [16384, 8], P('dev'), may hold values from 0 to 191
- next_bag: int32 [16384, 8], P('dev'), may hold values from 0 to 127
- hot_slots: int32 [4096], P('dev'), may hold values from 0 to 2047, as said below
- evict_dest: int32 [32, 32, 2], P('dev'), may hold values from -1 to 1023, as said below
- hot_cache: float32 [4096, 128], P('dev'), may hold values from -6 to 6
- evict_cache: float32 [2048, 128], P('dev'), may hold values from -6 to 6
- hot_table: float32 [2048, 128], P('dev'), may hold values from -6 to 6
- hot_accum: float32 [2048, 128], P('dev'), may hold values from 1 to 100
- owner_table: float32 [32768, 128], P('dev'), may hold values from -6 to 6
- owner_accum: float32 [32768, 128], P('dev'), may hold values from 1 to 30
- cross_w: float32 [2, 1024, 1024], P(None, None, 'dev'), may hold values from -0.1875 to 0.1875
- cross_b: float32 [2, 1024], P(None, 'dev'), may hold values from -3 to 3
- cross_accum: float32 [2, 1024, 1024], P(None, None, 'dev'), may hold values from 10000 to 1000000
Outputs:
- next_first: bfloat16 [16384, 1024], P('dev')
- hot_new: float32 [2048, 128], P('dev')
- hot_accum_new: float32 [2048, 128], P('dev')
- owner_new: float32 [32768, 128], P('dev')
- owner_accum_new: float32 [32768, 128], P('dev')
- cross_w_new: float32 [2, 1024, 1024], P(None, None, 'dev')
- cross_b_new: float32 [2, 1024], P(None, 'dev')
The draws below stay inside these ranges and needn't reach their ends.
Inputs may be any that keep to these rules, and one draw needn't show every extreme that they name: `hot_slots`: entry d * 128 + 4 * o + k names a row of owner o's block, o * 64 to o * 64 + 63; the 4 rows of one device in one owner's block are distinct. evict_dest[o, s, k] is the row of owner o's block (0 to 1023) that receives the gradient of source s's evicted slot 2 * o + k, or -1 for an empty slot; in each (o, s) bucket the live entries come first, and some bucket is full in every draw.
All inputs are finite; a program needn't handle non-finite values.
Results may differ from the reference program's by a relative error of at most 0.0033.
The reference program's roundings to bfloat16 on the way count: a program that leaves them out, or rounds other values in their place, can miss the bound.
Values may be sent and summed in bfloat16 or wider, within the bound.
No kernel may reach another device: no remote copies, remote signals or barrier semaphores. Data moves between devices by JAX's collectives and lax.ppermute only.
A program may use at most 128 MiB of HBM per device.

```python
import math
import jax
import jax.numpy as jnp
from jax import lax

E = 128
F = 8
D = 1024
TOK_DEV = 512
NEXT_DEV = 512
HB = 4
HOT_DEV = 64
EVB = 2
OWN_DEV = 1024
HOTC = 128
EVC = 64
HOT = 2048
OWNED = 32768
TOKENS = 16384
NEXT = 16384
N_DEV = 32


def draw_hot_slots(key, part):
    key_list = jax.random.split(jax.random.fold_in(key, 11), N_DEV * N_DEV)
    chosen = jax.vmap(lambda single: jax.random.permutation(single, HOT_DEV)[:HB])(key_list)
    owner_of = (jnp.arange(N_DEV * N_DEV) % N_DEV)[:, None]
    return (owner_of * HOT_DEV + chosen).reshape(-1).astype(jnp.int32)


def draw_evict_dest(key, part):
    first, second, third, fourth = jax.random.split(jax.random.fold_in(key, 23), 4)
    owner_heat = jax.random.randint(first, (N_DEV, 1), 0, 3)
    filled = jnp.minimum(EVB, jax.random.randint(second, (N_DEV, N_DEV), 0, EVB + 1) + owner_heat)
    corner = jax.random.randint(fourth, (2,), 0, N_DEV)
    filled = filled.at[corner[0], corner[1]].set(EVB)
    is_live = jnp.arange(EVB)[None, None, :] < filled[:, :, None]
    row_pick = jax.random.randint(third, (N_DEV, N_DEV, EVB), 0, OWN_DEV)
    return jnp.where(is_live, row_pick, -1).astype(jnp.int32)


def plant(result, own_key, least, largest):
    extent = result.shape
    place = [jax.random.randint(jax.random.fold_in(own_key, axis), (), 0, extent[axis]) for axis in range(len(extent))]
    result = result.at[tuple(place)].set(least)
    longest = extent.index(max(extent))
    place[longest] = (place[longest] + 1) % extent[longest]
    return result.at[tuple(place)].set(largest)


def with_spikes(values, own_key, source, target, shards_of, factor):
    def block_of(dim):
        return (jnp.arange(values.shape[dim]) // (values.shape[dim] // shards_of)).reshape((-1,) + (1,) * (values.ndim - 1 - dim))

    near = jax.random.permutation(own_key, shards_of)[block_of(target)]
    other_side = (block_of(target) + shards_of // 2) % shards_of
    return jnp.where((block_of(source) == near) | (block_of(source) == other_side), factor * values, values)


def level_of(rng, extent, pieces, low, largest):
    gain, own = 1.0, jax.random.fold_in(rng, 6)
    for axis_at, blocks in pieces:
        draws = jnp.exp(jax.random.uniform(jax.random.fold_in(own, axis_at), (blocks,), jnp.float32, low / len(pieces), largest / len(pieces)))
        gain = gain * jnp.repeat(draws, extent[axis_at] // blocks).reshape([-1 if axis == axis_at else 1 for axis in range(len(extent))])
    return gain


def centred(own_key, shape, scale, most, pieces=(), kind=jnp.bfloat16):
    array = scale * jax.random.normal(own_key, shape, jnp.float32)
    if pieces:
        array = array * level_of(own_key, shape, pieces, -0.22, 0.18)
    return jnp.clip(array, -most, most).astype(kind)


def heavy_noise(stream_key, extent, scale, bound, pieces, heavy, dtype=jnp.bfloat16):
    result = scale * jax.random.normal(stream_key, extent, jnp.float32)
    if pieces:
        result = result * level_of(stream_key, extent, pieces, -0.22, 0.18)
    return jnp.clip(with_spikes(result, jax.random.fold_in(stream_key, 3), *heavy), -bound, bound).astype(dtype)


def setup_inputs(seed: int = 0) -> dict:
    splits = jax.random.split(jax.random.key(seed), 15)
    return {
        "upstream": heavy_noise(splits[0], (TOKENS, D), 1.0, 6.0, ((0, 32),), (0, 1, 32, 2.75)),
        "bag": plant(jax.random.randint(splits[1], (TOKENS, F), 0, (HB + EVB) * N_DEV), jax.random.fold_in(splits[1], 1), 0, ((HB + EVB) * N_DEV) - 1).astype(jnp.int32),
        "next_bag": plant(jax.random.randint(splits[2], (NEXT, F), 0, HB * N_DEV), jax.random.fold_in(splits[2], 1), 0, (HB * N_DEV) - 1).astype(jnp.int32),
        "hot_slots": draw_hot_slots(jax.random.fold_in(splits[14], 71), 0),
        "evict_dest": draw_evict_dest(jax.random.fold_in(splits[14], 71), 0),
        "hot_cache": centred(splits[5], (N_DEV * HOTC, E), 1.0, 6.0, ((0, 32),), jnp.float32),
        "evict_cache": centred(splits[6], (N_DEV * EVC, E), 1.0, 6.0, ((0, 32),), jnp.float32),
        "hot_table": centred(splits[7], (HOT, E), 1.0, 6.0, ((0, 32),), jnp.float32),
        "hot_accum": jnp.clip(jnp.exp(math.log(100.0) - 4.6051702 * jax.random.uniform(splits[8], (HOT, E), jnp.float32) ** level_of(splits[8], (HOT, E), ((0, 32),), -0.2, 0.2)), 1.0, 100.0),
        "owner_table": centred(splits[9], (OWNED, E), 1.0, 6.0, ((0, 32),), jnp.float32),
        "owner_accum": jnp.clip(jnp.exp(math.log(30.0) - 3.4011974 * jax.random.uniform(splits[10], (OWNED, E), jnp.float32) ** level_of(splits[10], (OWNED, E), ((0, 32),), -0.2, 0.2)), 1.0, 30.0),
        "cross_w": centred(splits[11], (2, D, D), D ** -0.5, 0.1875, ((2, 32),), jnp.float32),
        "cross_b": centred(splits[12], (2, D), 0.5, 3.0, ((1, 32),), jnp.float32),
        "cross_accum": jnp.clip(jnp.exp(math.log(1000000) - 4.6051702 * jax.random.uniform(splits[13], (2, D, D), jnp.float32) ** level_of(splits[13], (2, D, D), ((2, 32),), -0.2, 0.2)), 10000.0, 1000000),
    }


row_rate = 0.05
weight_rate = 0.005
bias_rate = 0.0002
epsilon = 1e-10

def adagrad(params, accumulator, gradient, step_rate):
    updated = accumulator + gradient * gradient
    return (params - step_rate * gradient / (jnp.sqrt(updated) + epsilon), updated)

def rounded(values):
    return lax.optimization_barrier(values.astype(jnp.bfloat16)).astype(jnp.float32)

def device_pass(weights, biases, grad_in, bag_rows, slot_values):
    samples = bag_rows.shape[0]
    features = jnp.take(slot_values, bag_rows.reshape(-1), axis=0).reshape(samples, -1)
    feat_bf = features.astype(jnp.bfloat16)
    proj_one = jnp.dot(feat_bf, weights[0], preferred_element_type=jnp.float32) + biases[0]
    layer_one = features * proj_one + features
    layer_bf = layer_one.astype(jnp.bfloat16)
    proj_two = jnp.dot(layer_bf, weights[1], preferred_element_type=jnp.float32) + biases[1]
    grad_out = grad_in.astype(jnp.float32)
    grad_two = grad_out * features
    grad_two_bf = grad_two.astype(jnp.bfloat16)
    weight_two = jnp.dot(layer_bf.T, grad_two_bf, preferred_element_type=jnp.float32)
    bias_two = lax.optimization_barrier(jnp.sum(grad_two, axis=0))
    grad_layer = grad_out + jnp.dot(grad_two_bf, weights[1].T, preferred_element_type=jnp.float32)
    grad_one = grad_layer * features
    grad_one_bf = grad_one.astype(jnp.bfloat16)
    weight_one = jnp.dot(feat_bf.T, grad_one_bf, preferred_element_type=jnp.float32)
    bias_one = lax.optimization_barrier(jnp.sum(grad_one, axis=0))
    grad_feat = grad_out * proj_two + grad_layer * (proj_one + 1.0)
    grad_feat = grad_feat + jnp.dot(grad_one_bf, weights[0].T, preferred_element_type=jnp.float32)
    flat_grad = rounded(grad_feat).reshape(-1, slot_values.shape[1])
    slot_grad = jax.ops.segment_sum(flat_grad, bag_rows.reshape(-1), num_segments=slot_values.shape[0])
    return (weight_one, weight_two, bias_one, bias_two, slot_grad)

def reference(upstream, bag, next_bag, hot_slots, evict_dest, hot_cache, evict_cache, hot_table, hot_accum, owner_table, owner_accum, cross_w, cross_b, cross_accum):
    weights = cross_w.astype(jnp.bfloat16)
    biases = rounded(cross_b)
    hot_count = HB * N_DEV
    evict_count = EVB * N_DEV
    inputs = (upstream.reshape(N_DEV, TOK_DEV, D), bag.reshape(N_DEV, TOK_DEV, F), hot_cache.reshape(N_DEV, hot_count, E), evict_cache.reshape(N_DEV, evict_count, E), hot_slots.reshape(N_DEV, hot_count))

    def visit(carry, item):
        weight_sum, bias_sum, hot_grad = carry
        grad_in, bag_rows, hot_rows, evict_rows, hot_ids = item
        slot_values = jnp.concatenate([hot_rows, evict_rows], axis=0)
        weight_one, weight_two, bias_one, bias_two, slot_grad = device_pass(weights, biases, grad_in, bag_rows, slot_values)
        weight_sum = weight_sum + jnp.stack([weight_one, weight_two])
        bias_sum = bias_sum + jnp.stack([bias_one, bias_two])
        hot_grad = hot_grad.at[hot_ids].add(slot_grad[:hot_count])
        return ((weight_sum, bias_sum, hot_grad), slot_grad[hot_count:])
    start = (jnp.zeros((2, D, D), jnp.float32), jnp.zeros((2, D), jnp.float32), jnp.zeros((HOT_DEV * N_DEV, E), jnp.float32))
    (weight_sum, bias_sum, hot_grad), evicted = lax.scan(visit, start, inputs)
    hot_new, hot_accum_new = adagrad(hot_table, hot_accum, hot_grad, row_rate)
    moved = evicted.reshape(N_DEV, N_DEV, EVB, E).transpose(1, 0, 2, 3)
    owner_base = (jnp.arange(N_DEV).astype(jnp.int32) * OWN_DEV)[:, None, None]
    targets = jnp.where(evict_dest >= 0, owner_base + evict_dest, N_DEV * OWN_DEV).astype(jnp.int32)
    owner_grad = jax.ops.segment_sum(moved.reshape(-1, E), targets.reshape(-1), num_segments=N_DEV * OWN_DEV + 1)[:N_DEV * OWN_DEV]
    owner_new, owner_accum_new = adagrad(owner_table, owner_accum, owner_grad, row_rate)
    cross_w_new, unused = adagrad(cross_w, cross_accum, weight_sum, weight_rate)
    cross_b_new = cross_b - bias_rate * bias_sum
    held_rows = hot_new[hot_slots]
    slot_base = (jnp.arange(N_DEV).astype(jnp.int32) * hot_count)[:, None, None]
    picks = (slot_base + next_bag.reshape(N_DEV, NEXT_DEV, F)).astype(jnp.int32)
    next_feat = held_rows[picks.reshape(-1)].reshape(N_DEV * NEXT_DEV, D)
    proj = jnp.dot(next_feat.astype(jnp.bfloat16), cross_w_new[0].astype(jnp.bfloat16), preferred_element_type=jnp.float32) + rounded(cross_b_new[0])
    next_first = (next_feat * proj + next_feat).astype(jnp.bfloat16)
    return (next_first, hot_new, hot_accum_new, owner_new, owner_accum_new, cross_w_new, cross_b_new)
```

```python
import jax
import jax.numpy as jnp
import numpy as np
from jax import lax
from jax.sharding import PartitionSpec as P

row_rate = 0.05
weight_rate = 0.005
bias_rate = 0.0002
epsilon = 1e-10
f32 = jnp.float32
bf16 = jnp.bfloat16


def adagrad(params, accumulator, gradient, step_rate):
    updated = accumulator + gradient * gradient
    return (params - step_rate * gradient / (jnp.sqrt(updated) + epsilon), updated)


def bit_groups(devices):
    bits = devices.bit_length() - 1
    assert devices == 1 << bits
    return [(0, 1)] + [(low, min(2, bits - low)) for low in range(1, bits, 2)]


def group_masks(group):
    low, width = group
    return [value << low for value in range(1 << width)]


def relative_masks(devices):
    masks = [0]
    for group in reversed(bit_groups(devices)):
        masks = [own | inner for own in group_masks(group) for inner in masks]
    return np.array(masks, np.int32)


def swap(values, mask, devices):
    return lax.ppermute(values, "dev", [(i, i ^ mask) for i in range(devices)])


def gather_relative(block, devices):
    stack = block[None]
    for group in reversed(bit_groups(devices)):
        parts = [stack] + [swap(stack, mask, devices) for mask in group_masks(group)[1:]]
        stack = jnp.concatenate(parts, axis=0)
    return stack


def to_absolute(stack, my_index, devices):
    place = np.argsort(relative_masks(devices)).astype(np.int32)
    order = jnp.asarray(place)[jnp.arange(devices, dtype=jnp.int32) ^ my_index]
    return jnp.take(stack, order, axis=0, mode="clip").reshape(-1, stack.shape[-1])


def to_relative(blocks, my_index, devices):
    order = jnp.asarray(relative_masks(devices)) ^ my_index
    return jnp.take(blocks, order, axis=0, mode="clip")


def scatter_sum(stack, devices):
    for group in bit_groups(devices):
        masks = group_masks(group)
        parts = stack.reshape(len(masks), -1, *stack.shape[1:])
        total = parts[0].astype(f32)
        for k, mask in enumerate(masks[1:], 1):
            total = total + swap(parts[k].astype(bf16), mask, devices).astype(f32)
        stack = total
    return stack[0]


def split_rows(values):
    high = lax.reduce_precision(values, 8, 7)
    return jnp.concatenate([high, values - high], axis=1).astype(bf16)


def pick(one_hot, table):
    width = table.shape[1]
    both = split_rows(table)
    picked = [
        lax.dot_general(one_hot[k], both, (((0,), (0,)), ((), ())), preferred_element_type=f32)
        for k in range(one_hot.shape[0])
    ]
    high = jnp.concatenate([p[:, :width] for p in picked], axis=1)
    low = jnp.concatenate([p[:, width:] for p in picked], axis=1)
    return high + low, high.astype(bf16)


def one_hot_of(index, rows):
    return (
        index.T[:, None, :] == lax.broadcasted_iota(jnp.int32, (index.shape[1], rows, index.shape[0]), 1)
    ).astype(bf16)


def dot(a, b, ca, cb):
    return lax.dot_general(a, b, (((ca,), (cb,)), ((), ())), preferred_element_type=f32)


def exchange(values):
    return lax.all_to_all(values, "dev", split_axis=0, concat_axis=0, tiled=True)


def local(
    upstream,
    bag,
    next_bag,
    hot_slots,
    evict_dest,
    hot_cache,
    evict_cache,
    hot_table,
    hot_accum,
    owner_table,
    owner_accum,
    cross_w,
    cross_b,
    cross_accum,
):
    n = lax.axis_size("dev")
    me = lax.axis_index("dev")
    width = hot_cache.shape[1]
    fields = bag.shape[1]
    hot_count = hot_cache.shape[0]
    slots = hot_count + evict_cache.shape[0]
    columns = cross_b.shape[1]

    w_own = cross_w.transpose(0, 2, 1)
    w_send = w_own.astype(bf16)
    w1_rel = gather_relative(w_send[1], n)
    w0_rel = gather_relative(w_send[0], n)

    ids = hot_slots.reshape(n, -1)
    per = ids.shape[1]
    biases_own = cross_b.astype(bf16).astype(f32).reshape(1, -1)
    first = exchange(
        jnp.concatenate([ids.astype(f32), jnp.broadcast_to(biases_own, (n, 2 * columns))], axis=1)
    )
    arrived_ids = first[:, :per].astype(jnp.int32)
    biases = first[:, per:].reshape(n, 2, columns).transpose(1, 0, 2).reshape(2, -1)

    slot_values = jnp.concatenate([hot_cache, evict_cache], axis=0)
    one_hot = one_hot_of(bag, slots)
    feat, feat_bf = pick(one_hot, slot_values)
    g = upstream.astype(f32)
    grad_two = g * feat
    grad_two_bf = grad_two.astype(bf16)
    bias_two = jnp.sum(grad_two, axis=0)

    w1 = to_absolute(w1_rel, me, n)
    grad_layer = g + dot(grad_two_bf, w1, 1, 0)
    grad_one = grad_layer * feat
    grad_one_bf = grad_one.astype(bf16)
    bias_one = jnp.sum(grad_one, axis=0)
    weight_one = dot(grad_one_bf, feat_bf, 0, 0)
    grad0 = scatter_sum(to_relative(weight_one.reshape(n, columns, -1), me, n), n)
    w_new0, _ = adagrad(w_own[0], cross_accum.transpose(0, 2, 1)[0], grad0, weight_rate)
    wn_rel = gather_relative(w_new0.astype(bf16), n)

    w0 = to_absolute(w0_rel, me, n)
    proj_one = dot(feat_bf, w0, 1, 1) + biases[0]
    layer_one = feat * proj_one + feat
    layer_bf = layer_one.astype(bf16)
    weight_two = dot(grad_two_bf, layer_bf, 0, 0)
    grad1 = scatter_sum(to_relative(weight_two.reshape(n, columns, -1), me, n), n)
    w_new1, _ = adagrad(w_own[1], cross_accum.transpose(0, 2, 1)[1], grad1, weight_rate)
    proj_two = dot(layer_bf, w1, 1, 1) + biases[1]
    grad_feat = g * proj_two + grad_layer * (proj_one + 1.0) + dot(grad_one_bf, w0, 1, 0)
    grad_feat_bf = grad_feat.astype(bf16)
    slot_grad = sum(
        dot(one_hot[k], grad_feat_bf[:, k * width : (k + 1) * width], 1, 0) for k in range(fields)
    )

    bias_grads = jnp.stack([bias_one, bias_two]).reshape(2, n, columns).transpose(1, 0, 2)
    bias_row = jnp.pad(bias_grads.reshape(n, 1, -1), ((0, 0), (0, 0), (0, width - 2 * columns)))
    unpacked = exchange(
        jnp.concatenate(
            [
                slot_grad[:hot_count].reshape(n, -1, width),
                slot_grad[hot_count:].reshape(n, -1, width),
                bias_row,
            ],
            axis=1,
        )
    )
    arrived = unpacked[:, :per]
    moved = unpacked[:, per:-1]
    bias_sum = jnp.sum(unpacked[:, -1], axis=0)[: 2 * columns].reshape(2, columns)
    cross_b_new = cross_b - bias_rate * bias_sum

    local_rows = (arrived_ids - me * hot_table.shape[0]).reshape(-1)
    block_grad = jnp.zeros(hot_table.shape, f32).at[local_rows].add(arrived.reshape(-1, width))
    hot_new, hot_accum_new = adagrad(hot_table, hot_accum, block_grad, row_rate)
    returned = jnp.take(hot_new, local_rows, axis=0).reshape(n, -1, width)
    bias_back = jnp.pad(cross_b_new[0].astype(bf16).astype(f32), (0, width - columns))
    back = exchange(
        jnp.concatenate([returned, jnp.broadcast_to(bias_back, (n, 1, width))], axis=1)
    )
    held_rows = back[:, :-1].reshape(hot_count, width)
    next_bias = back[:, -1, :columns].reshape(-1)

    destination = evict_dest[0]
    targets = jnp.where(destination >= 0, destination, owner_table.shape[0]).reshape(-1)
    owner_grad = (
        jnp.zeros(owner_table.shape, f32).at[targets].add(moved.reshape(-1, width), mode="drop")
    )
    owner_new, owner_accum_new = adagrad(owner_table, owner_accum, owner_grad, row_rate)

    next_feat, next_bf = pick(one_hot_of(next_bag, hot_count), held_rows)
    wn = to_absolute(wn_rel, me, n)
    proj = dot(next_bf, wn, 1, 1) + next_bias
    next_first = (next_feat * proj + next_feat).astype(bf16)
    cross_w_new = jnp.stack([w_new0, w_new1]).transpose(0, 2, 1)
    return (
        next_first,
        hot_new,
        hot_accum_new,
        owner_new,
        owner_accum_new,
        cross_w_new,
        cross_b_new,
    )


def solution(mesh):
    return jax.shard_map(
        local,
        mesh=mesh,
        in_specs=(
            P("dev", None),
            P("dev", None),
            P("dev", None),
            P("dev"),
            P("dev", None, None),
            P("dev", None),
            P("dev", None),
            P("dev", None),
            P("dev", None),
            P("dev", None),
            P("dev", None),
            P(None, None, "dev"),
            P(None, "dev"),
            P(None, None, "dev"),
        ),
        out_specs=(
            P("dev", None),
            P("dev", None),
            P("dev", None),
            P("dev", None),
            P("dev", None),
            P(None, None, "dev"),
            P(None, "dev"),
        ),
        check_vma=False,
    )
```

```python
import math

import jax
import jax.numpy as jnp
import numpy as np
from jax import lax
from jax.experimental import pallas as pl
from jax.experimental.pallas import tpu as pltpu
from jax.sharding import PartitionSpec as P

row_rate = 0.05
weight_rate = 0.005
bias_rate = 0.0002
epsilon = 1e-10
f32 = jnp.float32
bf16 = jnp.bfloat16


def adagrad(params, accumulator, gradient, step_rate):
    updated = accumulator + gradient * gradient
    return (params - step_rate * gradient / (jnp.sqrt(updated) + epsilon), updated)


def bit_groups(devices):
    bits = devices.bit_length() - 1
    assert devices == 1 << bits
    return [(0, 1)] + [(low, min(2, bits - low)) for low in range(1, bits, 2)]


def group_masks(group):
    low, width = group
    return [value << low for value in range(1 << width)]


def relative_masks(devices):
    masks = [0]
    for group in reversed(bit_groups(devices)):
        masks = [own | inner for own in group_masks(group) for inner in masks]
    return np.array(masks, np.int32)


def swap(values, mask, devices):
    return lax.ppermute(values, "dev", [(i, i ^ mask) for i in range(devices)])


def after(values, *others):
    return lax.optimization_barrier((values, others))[0]


def gather_outer(block, devices):
    stack = block[None]
    for group in reversed(bit_groups(devices)[2:]):
        parts = [stack] + [swap(stack, mask, devices) for mask in group_masks(group)[1:]]
        stack = jnp.concatenate(parts, axis=0)
    return stack


def gather_near(stack, devices):
    near = [stack] + [swap(stack, m, devices) for m in group_masks(bit_groups(devices)[1])[1:]]
    return near + [swap(part, 1, devices) for part in near]


def sum_stage(keep, parts, group, devices):
    total = keep.astype(f32)
    arrived = [
        swap(part, mask, devices) for part, mask in zip(parts, group_masks(group)[1:])
    ]
    for part in arrived:
        total = total + part.astype(f32)
    return total, arrived


def parts_of(stack, group):
    parts = stack.reshape(len(group_masks(group)), -1, *stack.shape[1:])
    return parts[0], [parts[k].astype(bf16) for k in range(1, parts.shape[0])]


def to_absolute(parts, my_index, devices):
    stack = jnp.concatenate(parts, axis=0)
    place = np.argsort(relative_masks(devices)).astype(np.int32)
    order = jnp.asarray(place)[jnp.arange(devices, dtype=jnp.int32) ^ my_index]
    return jnp.take(stack, order, axis=0, mode="clip").reshape(-1, stack.shape[-1])


def to_relative(blocks, my_index, devices):
    order = jnp.asarray(relative_masks(devices)) ^ my_index
    return jnp.take(blocks, order, axis=0, mode="clip")


def dot(a, b, ca, cb):
    return lax.dot_general(a, b, (((ca,), (cb,)), ((), ())), preferred_element_type=f32)


def exchange(values):
    return lax.all_to_all(values, "dev", split_axis=0, concat_axis=0, tiled=True)


def one_hot(index_row, rows):
    samples = index_row.shape[1]
    return (index_row == lax.broadcasted_iota(jnp.int32, (rows, samples), 0)).astype(bf16)


def high_low(table):
    high = table.astype(bf16)
    return jnp.concatenate([high, (table - high.astype(f32)).astype(bf16)], axis=1)


def call(body, outs, inputs, scratch=(), loose=(), name=None):
    vmem = pl.BlockSpec(memory_space=pltpu.VMEM)
    count = len(inputs)

    def kernel(*refs):
        body(*refs[:count], *refs[count + len(loose) :])

    return pl.pallas_call(
        kernel,
        out_shape=[jax.ShapeDtypeStruct(*out) for out in outs],
        in_specs=[pl.BlockSpec(memory_space=pltpu.SMEM)]
        + [vmem] * (count - 1)
        + [pl.BlockSpec(memory_space=pl.ANY)] * len(loose),
        out_specs=[vmem] * len(outs),
        scratch_shapes=[pltpu.VMEM(*shape) for shape in scratch],
        name=name,
    )(*inputs, *loose)


def put_parts(parts, target, my_index, masks):
    place = 0
    for part in parts:
        for k in range(part.shape[0]):
            target[masks[place] ^ my_index] = part[k]
            place += 1


def give_halves(blocks, keep, send, my_index, masks):
    half = len(masks) // 2
    for place in range(half):
        keep[place] = blocks[masks[place] ^ my_index]
        send[place] = blocks[masks[half + place] ^ my_index].astype(bf16)


def chunks(rows):
    step = math.gcd(rows, 256)
    return [slice(at, at + step) for at in range(0, rows, step)]


def pick(me, index, table, loose=()):
    fields, samples = index.shape
    rows, width = table.shape

    def body(me_ref, index_ref, table_ref, out):
        both = high_low(table_ref[...])
        for k in range(fields):
            picked = dot(one_hot(index_ref[k : k + 1, :], rows), both, 0, 0)
            out[:, k * width : (k + 1) * width] = picked[:, :width] + picked[:, width:]

    return call(
        body, [((samples, fields * width), f32)], [me, index, table], loose=loose, name="pick"
    )[0]


def step_two(me, masks, parts, upstream, feat):
    n, r, depth = len(masks), parts[0].shape[1], feat.shape[1]
    samples = feat.shape[0]

    def body(me_ref, up, feat_ref, *refs):
        refs = list(refs)
        part_refs, refs = refs[: len(parts)], refs[len(parts) :]
        layer, one_bf, bias, w1, keep, send, feat_bf, grads = refs
        mine = me_ref[0]
        put_parts(part_refs, w1, mine, masks)
        weights = w1[...].reshape(n * r, depth)
        total = jnp.zeros((1, depth), f32)
        for at in chunks(samples):
            g = up[at].astype(f32)
            f = feat_ref[at]
            feat_bf[at] = f.astype(bf16)
            grad_layer = g + dot((g * f).astype(bf16), weights, 1, 0)
            layer[at] = grad_layer
            grad_one = grad_layer * f
            total = total + jnp.sum(grad_one, axis=0, keepdims=True)
            one_bf[at] = grad_one.astype(bf16)
        bias[...] = total
        grads[...] = dot(one_bf[...], feat_bf[...], 0, 0).reshape(n, r, depth)
        give_halves(grads, keep, send, mine, masks)

    return call(
        body,
        [
            ((samples, depth), f32),
            ((samples, depth), bf16),
            ((1, depth), f32),
            ((n, r, depth), bf16),
            ((n // 2, r, depth), f32),
            ((n // 2, r, depth), bf16),
        ],
        [me, upstream, feat, *parts],
        [((samples, depth), bf16), ((n, r, depth), f32)],
        name="step_two",
    )


def step_four(me, masks, parts, upstream, feat, layer, one_bf, w1, biases, index, slots, loose):
    n, r, depth = len(masks), parts[0].shape[1], feat.shape[1]
    samples, fields = feat.shape[0], index.shape[0]
    width = depth // fields

    def body(me_ref, up, feat_ref, layer_ref, one_ref, w1_ref, biases_ref, index_ref, *refs):
        refs = list(refs)
        part_refs, refs = refs[: len(parts)], refs[len(parts) :]
        slot, bias, keep, send, w0, layer_bf, two_bf, feat_grad, grads = refs
        mine = me_ref[0]
        put_parts(part_refs, w0, mine, masks)
        first = w0[...].reshape(n * r, depth)
        second = w1_ref[...].reshape(n * r, depth)
        total = jnp.zeros((1, depth), f32)
        for at in chunks(samples):
            g = up[at].astype(f32)
            f = feat_ref[at]
            two = g * f
            total = total + jnp.sum(two, axis=0, keepdims=True)
            two_bf[at] = two.astype(bf16)
            proj_one = dot(f.astype(bf16), first, 1, 1) + biases_ref[0:1]
            layer_bf[at] = (f * proj_one + f).astype(bf16)
            proj_two = dot(layer_bf[at], second, 1, 1) + biases_ref[1:2]
            grad_feat = g * proj_two + layer_ref[at] * (proj_one + 1.0)
            grad_feat = grad_feat + dot(one_ref[at], first, 1, 0)
            feat_grad[at] = grad_feat.astype(bf16)
        bias[...] = total
        slot_sum = jnp.zeros((slots, width), f32)
        for k in range(fields):
            block = feat_grad[:, k * width : (k + 1) * width]
            slot_sum = slot_sum + dot(one_hot(index_ref[k : k + 1, :], slots), block, 1, 0)
        slot[...] = slot_sum
        grads[...] = dot(two_bf[...], layer_bf[...], 0, 0).reshape(n, r, depth)
        give_halves(grads, keep, send, mine, masks)

    return call(
        body,
        [
            ((slots, width), f32),
            ((1, depth), f32),
            ((n // 2, r, depth), f32),
            ((n // 2, r, depth), bf16),
        ],
        [me, upstream, feat, layer, one_bf, w1, biases, index, *parts],
        [
            ((n, r, depth), bf16),
            ((samples, depth), bf16),
            ((samples, depth), bf16),
            ((samples, depth), bf16),
            ((n, r, depth), f32),
        ],
        loose,
        name="step_four",
    )


def step_six(me, masks, parts, feat, bias):
    n, r, depth = len(masks), parts[0].shape[1], feat.shape[1]
    samples = feat.shape[0]

    def body(me_ref, feat_ref, bias_ref, *refs):
        part_refs, (out, wn) = refs[: len(parts)], refs[len(parts) :]
        put_parts(part_refs, wn, me_ref[0], masks)
        weights = wn[...].reshape(n * r, depth)
        for at in chunks(samples):
            f = feat_ref[at]
            proj = dot(f.astype(bf16), weights, 1, 1) + bias_ref[...]
            out[at] = (f * proj + f).astype(bf16)

    return call(
        body,
        [((samples, depth), bf16)],
        [me, feat, bias, *parts],
        [((n, r, depth), bf16)],
        name="step_six",
    )[0]


def plain_pick(me, index, table, loose=()):
    both = high_low(lax.optimization_barrier(table))
    width = table.shape[1]
    picked = [dot(one_hot(row[None], table.shape[0]), both, 0, 0) for row in index]
    return jnp.concatenate([p[:, :width] + p[:, width:] for p in picked], axis=1)


def plain_halves(grads, me, masks):
    n = len(masks)
    placed = to_relative(grads.reshape(n, -1, grads.shape[1]), me[0], n)
    return placed[: n // 2], placed[n // 2 :].astype(bf16)


def plain_two(me, masks, parts, upstream, feat):
    w1 = to_absolute(parts, me[0], len(masks))
    g = upstream.astype(f32)
    layer = g + dot((g * feat).astype(bf16), w1, 1, 0)
    grad_one = layer * feat
    one_bf = grad_one.astype(bf16)
    keep, send = plain_halves(dot(one_bf, feat.astype(bf16), 0, 0), me, masks)
    return layer, one_bf, jnp.sum(grad_one, axis=0, keepdims=True), w1, keep, send


def plain_four(me, masks, parts, upstream, feat, layer, one_bf, w1, biases, index, slots, loose):
    w0 = to_absolute(parts, me[0], len(masks))
    g = upstream.astype(f32)
    two = g * feat
    proj_one = dot(feat.astype(bf16), w0, 1, 1) + biases[0:1]
    layer_bf = (feat * proj_one + feat).astype(bf16)
    proj_two = dot(layer_bf, w1, 1, 1) + biases[1:2]
    grad_feat = g * proj_two + layer * (proj_one + 1.0) + dot(one_bf, w0, 1, 0)
    grad_feat = grad_feat.astype(bf16)
    width = feat.shape[1] // index.shape[0]
    slot = sum(
        dot(one_hot(row[None], slots), grad_feat[:, k * width : (k + 1) * width], 1, 0)
        for k, row in enumerate(index)
    )
    keep, send = plain_halves(dot(two.astype(bf16), layer_bf, 0, 0), me, masks)
    return slot, jnp.sum(two, axis=0, keepdims=True), keep, send


def plain_six(me, masks, parts, feat, bias):
    wn = to_absolute(parts, me[0], len(masks))
    proj = dot(feat.astype(bf16), wn, 1, 1) + bias
    return (feat * proj + feat).astype(bf16)


def local(
    upstream,
    bag,
    next_bag,
    hot_slots,
    evict_dest,
    hot_cache,
    evict_cache,
    hot_table,
    hot_accum,
    owner_table,
    owner_accum,
    cross_w,
    cross_b,
    cross_accum,
):
    n = lax.axis_size("dev")
    me = lax.axis_index("dev")
    width = hot_cache.shape[1]
    fields = bag.shape[1]
    hot_count = hot_cache.shape[0]
    slots = hot_count + evict_cache.shape[0]
    columns = cross_b.shape[1]

    place = me.astype(jnp.int32).reshape(1)
    masks = [int(mask) for mask in relative_masks(n)]
    groups = bit_groups(n)
    if columns % 16 == 0 and bag.shape[0] % 128 == 0:
        take, two, four, six = pick, step_two, step_four, step_six
    else:
        take, two, four, six = plain_pick, plain_two, plain_four, plain_six

    w_own = cross_w.transpose(0, 2, 1)
    w1_outer = gather_outer(w_own[1].astype(bf16), n)
    w1_parts = gather_near(w1_outer, n)
    w0_outer = gather_outer(after(w_own[0].astype(bf16), w1_outer), n)
    w0_parts = gather_near(after(w0_outer, *w1_parts[: len(w1_parts) // 2]), n)

    ids = hot_slots.reshape(n, -1)
    per = ids.shape[1]
    biases_own = cross_b.astype(bf16).astype(f32).reshape(1, -1)
    first = exchange(
        after(
            jnp.concatenate(
                [ids.astype(f32), jnp.broadcast_to(biases_own, (n, 2 * columns))], axis=1
            ),
            w1_outer,
        )
    )
    arrived_ids = first[:, :per].astype(jnp.int32)
    biases = first[:, per:].reshape(n, 2, columns).transpose(1, 0, 2).reshape(2, -1)

    slot_values = jnp.concatenate([hot_cache, evict_cache], axis=0)
    feat = take(place, bag.T, slot_values, (w1_outer,))

    def near_sum(keep, send):
        total, _ = sum_stage(keep, [send], groups[0], n)
        return parts_of(total, groups[1])

    def own_sum(total):
        for group in groups[2:]:
            keep, parts = parts_of(total, group)
            total, _ = sum_stage(keep, parts, group, n)
        return total[0]

    layer, one_bf, bias_one, w1, keep0, send0 = two(place, masks, w1_parts, upstream, feat)
    keep0, parts0 = near_sum(keep0, send0)
    slot_grad, bias_two, keep1, send1 = four(
        place, masks, w0_parts, upstream, feat, layer, one_bf, w1, biases, bag.T, slots, parts0
    )
    total0, arrived0 = sum_stage(keep0, parts0, groups[1], n)
    grad0 = own_sum(total0)
    w_new0, _ = adagrad(w_own[0], cross_accum.transpose(0, 2, 1)[0], grad0, weight_rate)
    wn_outer = gather_outer(w_new0.astype(bf16), n)
    wn_parts = gather_near(wn_outer, n)

    keep1, parts1 = near_sum(keep1, send1)
    total1, _ = sum_stage(keep1, after(parts1, *arrived0), groups[1], n)
    grad1 = own_sum(after(total1, wn_outer))
    w_new1, _ = adagrad(w_own[1], cross_accum.transpose(0, 2, 1)[1], grad1, weight_rate)

    bias_grads = jnp.concatenate([bias_one, bias_two]).reshape(2, n, columns).transpose(1, 0, 2)
    bias_row = jnp.pad(bias_grads.reshape(n, 1, -1), ((0, 0), (0, 0), (0, width - 2 * columns)))
    unpacked = exchange(
        jnp.concatenate(
            [
                slot_grad[:hot_count].reshape(n, -1, width),
                slot_grad[hot_count:].reshape(n, -1, width),
                bias_row,
            ],
            axis=1,
        )
    )
    unpacked = after(unpacked, total0)
    arrived = unpacked[:, :per]
    moved = unpacked[:, per:-1]
    bias_sum = jnp.sum(unpacked[:, -1], axis=0)[: 2 * columns].reshape(2, columns)
    cross_b_new = cross_b - bias_rate * bias_sum

    local_rows = (arrived_ids - me * hot_table.shape[0]).reshape(-1)
    block_grad = jnp.zeros(hot_table.shape, f32).at[local_rows].add(arrived.reshape(-1, width))
    hot_new, hot_accum_new = adagrad(hot_table, hot_accum, block_grad, row_rate)
    returned = jnp.take(hot_new, local_rows, axis=0).reshape(n, -1, width)
    bias_back = jnp.pad(cross_b_new[0].astype(bf16).astype(f32), (0, width - columns))
    back = exchange(
        jnp.concatenate([returned, jnp.broadcast_to(bias_back, (n, 1, width))], axis=1)
    )
    held_rows = back[:, :-1].reshape(hot_count, width)
    next_bias = back[:, -1, :columns].reshape(-1)

    moved = after(moved, w_new0)
    destination = evict_dest[0]
    targets = jnp.where(destination >= 0, destination, owner_table.shape[0]).reshape(-1)
    owner_grad = (
        jnp.zeros(owner_table.shape, f32).at[targets].add(moved.reshape(-1, width), mode="drop")
    )
    owner_new, owner_accum_new = adagrad(owner_table, owner_accum, owner_grad, row_rate)

    next_feat = take(place, next_bag.T, held_rows)
    next_first = six(place, masks, wn_parts, next_feat, next_bias[None])
    cross_w_new = jnp.stack([w_new0, w_new1]).transpose(0, 2, 1)
    return (
        next_first,
        hot_new,
        hot_accum_new,
        owner_new,
        owner_accum_new,
        cross_w_new,
        cross_b_new,
    )


def solution(mesh):
    return jax.shard_map(
        local,
        mesh=mesh,
        in_specs=(
            P("dev", None),
            P("dev", None),
            P("dev", None),
            P("dev"),
            P("dev", None, None),
            P("dev", None),
            P("dev", None),
            P("dev", None),
            P("dev", None),
            P("dev", None),
            P("dev", None),
            P(None, None, "dev"),
            P(None, "dev"),
            P(None, None, "dev"),
        ),
        out_specs=(
            P("dev", None),
            P("dev", None),
            P("dev", None),
            P("dev", None),
            P("dev", None),
            P(None, None, "dev"),
            P(None, "dev"),
        ),
        check_vma=False,
    )
```

```python
import math

import jax
import jax.numpy as jnp
import numpy as np
from jax import lax
from jax.experimental import pallas as pl
from jax.experimental.pallas import tpu as pltpu
from jax.sharding import PartitionSpec as P


row_rate = 0.05
weight_rate = 0.005
bias_rate = 0.0002
epsilon = 1e-10
f32 = jnp.float32
bf16 = jnp.bfloat16


def adagrad(params, accumulator, gradient, step_rate):
    updated = accumulator + gradient * gradient
    return (params - step_rate * gradient / (jnp.sqrt(updated) + epsilon), updated)


def bit_groups(devices):
    bits = devices.bit_length() - 1
    assert devices == 1 << bits
    return [(0, 1)] + [(low, min(2, bits - low)) for low in range(1, bits, 2)]


def group_masks(group):
    low, width = group
    return [value << low for value in range(1 << width)]


def relative_masks(devices):
    masks = [0]
    for group in reversed(bit_groups(devices)):
        masks = [own | inner for own in group_masks(group) for inner in masks]
    return np.array(masks, np.int32)


def swap(values, mask, devices):
    return lax.ppermute(values, "dev", [(i, i ^ mask) for i in range(devices)])


def after(values, *others):
    return lax.optimization_barrier((values, others))[0]


def gather_outer(block, devices):
    stack = block[None]
    for group in reversed(bit_groups(devices)[2:]):
        parts = [stack] + [swap(stack, mask, devices) for mask in group_masks(group)[1:]]
        stack = jnp.concatenate(parts, axis=0)
    return stack


def gather_near(stack, devices):
    masks = group_masks(bit_groups(devices)[1])[1:]
    near = [stack] + [swap(stack, mask, devices) for mask in masks]
    return near + [swap(part, 1, devices) for part in near]


def sum_stage(keep, parts, group, devices):
    total = keep.astype(f32)
    arrived = [swap(part, mask, devices) for part, mask in zip(parts, group_masks(group)[1:])]
    for part in arrived:
        total = total + part.astype(f32)
    return total, arrived


def parts_of(stack, group):
    parts = stack.reshape(len(group_masks(group)), -1, *stack.shape[1:])
    return parts[0], [parts[k].astype(bf16) for k in range(1, parts.shape[0])]


def to_absolute(parts, my_index, devices):
    stack = jnp.concatenate(parts, axis=0)
    place = np.argsort(relative_masks(devices)).astype(np.int32)
    order = jnp.asarray(place)[jnp.arange(devices, dtype=jnp.int32) ^ my_index]
    return jnp.take(stack, order, axis=0, mode="clip").reshape(-1, stack.shape[-1])


def to_relative(blocks, my_index, devices):
    order = jnp.asarray(relative_masks(devices)) ^ my_index
    return jnp.take(blocks, order, axis=0, mode="clip")


def dot(a, b, ca, cb):
    return lax.dot_general(a, b, (((ca,), (cb,)), ((), ())), preferred_element_type=f32)


def exchange(values):
    return lax.all_to_all(values, "dev", split_axis=0, concat_axis=0, tiled=True)


def one_hot(index_row, rows):
    samples = index_row.shape[1]
    return (index_row == lax.broadcasted_iota(jnp.int32, (rows, samples), 0)).astype(bf16)


def high_low(table):
    high = table.astype(bf16)
    return jnp.concatenate([high, (table - high.astype(f32)).astype(bf16)], axis=1)


def call(body, outs, inputs, scratch=(), loose=()):
    vmem = pl.BlockSpec(memory_space=pltpu.VMEM)
    count = len(inputs)

    def kernel(*refs):
        body(*refs[:count], *refs[count + len(loose) :])

    return pl.pallas_call(
        kernel,
        out_shape=[jax.ShapeDtypeStruct(*out) for out in outs],
        in_specs=[pl.BlockSpec(memory_space=pltpu.SMEM)]
        + [vmem] * (count - 1)
        + [pl.BlockSpec(memory_space=pl.ANY)] * len(loose),
        out_specs=[vmem] * len(outs),
        scratch_shapes=[pltpu.VMEM(*shape) for shape in scratch],
    )(*inputs, *loose)


def put_parts(parts, target, my_index, masks):
    place = 0
    for part in parts:
        for k in range(part.shape[0]):
            target[masks[place] ^ my_index] = part[k]
            place += 1


def give_halves(blocks, keep, send, my_index, masks):
    half = len(masks) // 2
    for place in range(half):
        keep[place] = blocks[masks[place] ^ my_index]
        send[place] = blocks[masks[half + place] ^ my_index].astype(bf16)


def chunks(rows):
    step = math.gcd(rows, 256)
    return [slice(at, at + step) for at in range(0, rows, step)]


def pick(me, index, table, loose=()):
    fields, samples = index.shape
    rows, width = table.shape

    def body(me_ref, index_ref, table_ref, out):
        both = high_low(table_ref[...])
        for k in range(fields):
            picked = dot(one_hot(index_ref[k : k + 1, :], rows), both, 0, 0)
            out[:, k * width : (k + 1) * width] = picked[:, :width] + picked[:, width:]

    return call(body, [((samples, fields * width), f32)], [me, index, table], loose=loose)[0]


def step_two(me, masks, parts, upstream, feat):
    n, r, depth = len(masks), parts[0].shape[1], feat.shape[1]
    samples = feat.shape[0]

    def body(me_ref, up, feat_ref, *refs):
        refs = list(refs)
        part_refs, refs = refs[: len(parts)], refs[len(parts) :]
        bias, keep, send, w1, one_bf, feat_bf, grads = refs
        mine = me_ref[0]
        put_parts(part_refs, w1, mine, masks)
        weights = w1[...].reshape(n * r, depth)
        total = jnp.zeros((1, depth), f32)
        for at in chunks(samples):
            g = up[at].astype(f32)
            f = feat_ref[at]
            feat_bf[at] = f.astype(bf16)
            grad_layer = g + dot((g * f).astype(bf16), weights, 1, 0)
            grad_one = grad_layer * f
            total = total + jnp.sum(grad_one, axis=0, keepdims=True)
            one_bf[at] = grad_one.astype(bf16)
        bias[...] = total
        grads[...] = dot(one_bf[...], feat_bf[...], 0, 0).reshape(n, r, depth)
        give_halves(grads, keep, send, mine, masks)

    return call(
        body,
        [
            ((1, depth), f32),
            ((n // 2, r, depth), f32),
            ((n // 2, r, depth), bf16),
        ],
        [me, upstream, feat, *parts],
        [
            ((n, r, depth), bf16),
            ((samples, depth), bf16),
            ((samples, depth), bf16),
            ((n, r, depth), f32),
        ],
    )


def iota(shape, dim):
    return lax.broadcasted_iota(jnp.int32, shape, dim)


def log2(count):
    assert count & (count - 1) == 0
    return count.bit_length() - 1


class Packing:
    def __init__(self, devices, shared, evicted, columns):
        self.devices, self.shared, self.evicted = devices, shared, evicted
        self.columns = columns
        self.bias_row = shared + evicted
        self.each = 8 << max(0, (self.bias_row // 8).bit_length())
        self.total = devices * self.each

    def pack(self, slot_sum, biases):
        width = slot_sum.shape[1]
        shape = (self.total, slot_sum.shape[0])
        device, row = iota(shape, 0) >> log2(self.each), iota(shape, 0) & (self.each - 1)
        evict = self.devices * self.shared + device * self.evicted + row - self.shared
        slot = jnp.where(row < self.shared, device * self.shared + row, evict)
        slot = jnp.where(row < self.bias_row, slot, -1)
        chosen = (slot == iota(shape, 1)).astype(bf16)
        packed = halves_sum(dot(chosen, high_low(slot_sum), 1, 0), width)
        spread = jnp.zeros((self.devices, width), f32)
        for layer, bias in enumerate(biases):
            depth = bias.shape[1]
            shape = (self.devices, depth)
            own = jnp.where(iota(shape, 1) >> log2(self.columns) == iota(shape, 0), bias, 0.0)
            shape = (depth, width)
            lane = (iota(shape, 0) & (self.columns - 1)) + layer * self.columns
            to = (lane == iota(shape, 1)).astype(bf16)
            high = own.astype(bf16)
            low = (own - high.astype(f32)).astype(bf16)
            spread = spread + dot(high, to, 1, 0) + dot(low, to, 1, 0)
        shape = (self.total, self.devices)
        here = iota(shape, 0) == (iota(shape, 1) << log2(self.each)) + self.bias_row
        return packed + halves_sum(dot(here.astype(bf16), high_low(spread), 1, 0), width)

    def rows(self, values, at):
        after_them = self.each - at - values.shape[1]
        spaced = jnp.pad(values, ((0, 0), (at, after_them)), constant_values=-1)
        return spaced.reshape(1, -1)


def step_four(me, masks, parts, parts1, upstream, feat, biases, index, slots, bias1, packing, loose):
    n, r, depth = len(masks), parts[0].shape[1], feat.shape[1]
    samples, fields = feat.shape[0], index.shape[0]
    width = depth // fields

    def body(me_ref, up, feat_ref, biases_ref, index_ref, bias1_ref, *refs):
        refs = list(refs)
        count = len(parts)
        packed, keep, send, w0, w1, layer_bf, two_bf, feat_grad, grads = refs[2 * count :]
        mine = me_ref[0]
        put_parts(refs[:count], w0, mine, masks)
        put_parts(refs[count : 2 * count], w1, mine, masks)
        first = w0[...].reshape(n * r, depth)
        second = w1[...].reshape(n * r, depth)
        total = jnp.zeros((1, depth), f32)
        for at in chunks(samples):
            g = up[at].astype(f32)
            f = feat_ref[at]
            two = g * f
            total = total + jnp.sum(two, axis=0, keepdims=True)
            two_bf[at] = two.astype(bf16)
            proj_one = dot(f.astype(bf16), first, 1, 1) + biases_ref[0:1]
            layer_bf[at] = (f * proj_one + f).astype(bf16)
            proj_two = dot(layer_bf[at], second, 1, 1) + biases_ref[1:2]
            layer = g + dot(two_bf[at], second, 1, 0)
            grad_feat = g * proj_two + layer * (proj_one + 1.0)
            grad_feat = grad_feat + dot((layer * f).astype(bf16), first, 1, 0)
            feat_grad[at] = grad_feat.astype(bf16)
        slot_sum = jnp.zeros((slots, width), f32)
        for k in range(fields):
            block = feat_grad[:, k * width : (k + 1) * width]
            slot_sum = slot_sum + dot(one_hot(index_ref[k : k + 1, :], slots), block, 1, 0)
        packed[...] = packing.pack(slot_sum, (bias1_ref[...], total))
        grads[...] = dot(two_bf[...], layer_bf[...], 0, 0).reshape(n, r, depth)
        give_halves(grads, keep, send, mine, masks)

    return call(
        body,
        [
            ((packing.total, width), f32),
            ((n // 2, r, depth), f32),
            ((n // 2, r, depth), bf16),
        ],
        [me, upstream, feat, biases, index, bias1, *parts, *parts1],
        [
            ((n, r, depth), bf16),
            ((n, r, depth), bf16),
            ((samples, depth), bf16),
            ((samples, depth), bf16),
            ((samples, depth), bf16),
            ((n, r, depth), f32),
        ],
        loose,
    )


def step_six(me, masks, parts, feat, bias):
    n, r, depth = len(masks), parts[0].shape[1], feat.shape[1]
    samples = feat.shape[0]

    def body(me_ref, feat_ref, bias_ref, *refs):
        part_refs, (out, wn) = refs[: len(parts)], refs[len(parts) :]
        put_parts(part_refs, wn, me_ref[0], masks)
        weights = wn[...].reshape(n * r, depth)
        for at in chunks(samples):
            f = feat_ref[at]
            proj = dot(f.astype(bf16), weights, 1, 1) + bias_ref[...]
            out[at] = (f * proj + f).astype(bf16)

    return call(
        body, [((samples, depth), bf16)], [me, feat, bias, *parts], [((n, r, depth), bf16)]
    )[0]


def halves_sum(both, width):
    return both[:, :width] + both[:, width:]


def hot_update(me, rows, arrived, table, accum, bias, packing):
    width = table.shape[1]

    def body(me_ref, rows_ref, arrived_ref, table_ref, accum_ref, bias_ref, *outs):
        new, accum_new, returned, bias_new = outs
        values = arrived_ref[...]
        place = iota(values.shape, 0) & (packing.each - 1)
        bias_sum = jnp.where(place == packing.bias_row, values, 0.0)
        bias_sum = jnp.sum(bias_sum, axis=0, keepdims=True)
        stepped = bias_ref[...] - bias_rate * bias_sum
        bias_new[...] = stepped
        chosen = one_hot(rows_ref[...], table.shape[0])
        gradient = halves_sum(dot(chosen, high_low(values), 1, 0), width)
        updated, accum_new[...] = adagrad(table_ref[...], accum_ref[...], gradient, row_rate)
        new[...] = updated
        back = halves_sum(dot(chosen, high_low(updated), 0, 0), width)
        returned[...] = jnp.where(
            place == packing.bias_row, stepped.astype(bf16).astype(f32), back
        )

    return call(
        body,
        [(table.shape, f32), (table.shape, f32), (arrived.shape, f32), ((1, width), f32)],
        [me, rows, arrived, table, accum, bias],
    )


def pick_next(me, index, table, packing, depth):
    fields, samples = index.shape
    rows, width = table.shape

    def body(me_ref, index_ref, table_ref, out, bias):
        values = table_ref[...]
        both = high_low(values)
        for k in range(fields):
            picked = dot(one_hot(index_ref[k : k + 1, :], rows), both, 0, 0)
            out[:, k * width : (k + 1) * width] = halves_sum(picked, width)
        shape = (width, depth)
        lanes = (iota(shape, 1) & (packing.columns - 1)) == iota(shape, 0)
        spread = dot(values.astype(bf16), lanes.astype(bf16), 1, 0)
        shape = (rows, depth)
        device = iota(shape, 1) >> log2(packing.columns)
        here = iota(shape, 0) == (device << log2(packing.each)) + packing.bias_row
        bias[...] = jnp.sum(jnp.where(here, spread, 0.0), axis=0, keepdims=True)

    return call(body, [((samples, depth), f32), ((1, depth), f32)], [me, index, table])


def owner_update(me, rows, moved, table, accum):
    width = table.shape[1]

    def body(me_ref, rows_ref, moved_ref, table_ref, accum_ref, new, accum_new):
        chosen = one_hot(rows_ref[...], table.shape[0])
        gradient = halves_sum(dot(chosen, high_low(moved_ref[...]), 1, 0), width)
        new[...], accum_new[...] = adagrad(table_ref[...], accum_ref[...], gradient, row_rate)

    return call(body, [(table.shape, f32), (table.shape, f32)], [me, rows, moved, table, accum])


def plain_halves(grads, me, masks):
    n = len(masks)
    placed = to_relative(grads.reshape(n, -1, grads.shape[1]), me[0], n)
    return placed[: n // 2], placed[n // 2 :].astype(bf16)


def plain_two(me, masks, parts, upstream, feat):
    w1 = to_absolute(parts, me[0], len(masks))
    g = upstream.astype(f32)
    layer = g + dot((g * feat).astype(bf16), w1, 1, 0)
    grad_one = layer * feat
    one_bf = grad_one.astype(bf16)
    keep, send = plain_halves(dot(one_bf, feat.astype(bf16), 0, 0), me, masks)
    return jnp.sum(grad_one, axis=0, keepdims=True), keep, send


def plain_four(me, masks, parts, parts1, upstream, feat, biases, index, slots, bias1, packing, loose):
    w0 = to_absolute(parts, me[0], len(masks))
    w1 = to_absolute(parts1, me[0], len(masks))
    g = upstream.astype(f32)
    two = g * feat
    proj_one = dot(feat.astype(bf16), w0, 1, 1) + biases[0:1]
    layer_bf = (feat * proj_one + feat).astype(bf16)
    proj_two = dot(layer_bf, w1, 1, 1) + biases[1:2]
    layer = g + dot(two.astype(bf16), w1, 1, 0)
    one_bf = (layer * feat).astype(bf16)
    grad_feat = g * proj_two + layer * (proj_one + 1.0) + dot(one_bf, w0, 1, 0)
    grad_feat = grad_feat.astype(bf16)
    width = feat.shape[1] // index.shape[0]
    slot = sum(
        dot(one_hot(row[None], slots), grad_feat[:, k * width : (k + 1) * width], 1, 0)
        for k, row in enumerate(index)
    )
    keep, send = plain_halves(dot(two.astype(bf16), layer_bf, 0, 0), me, masks)
    packed = packing.pack(slot, (bias1, jnp.sum(two, axis=0, keepdims=True)))
    return packed, keep, send


def plain_six(me, masks, parts, feat, bias):
    wn = to_absolute(parts, me[0], len(masks))
    proj = dot(feat.astype(bf16), wn, 1, 1) + bias
    return (feat * proj + feat).astype(bf16)


def local(
    upstream,
    bag,
    next_bag,
    hot_slots,
    evict_dest,
    hot_cache,
    evict_cache,
    hot_table,
    hot_accum,
    owner_table,
    owner_accum,
    cross_w,
    cross_b,
    cross_accum,
):
    n = lax.axis_size("dev")
    me = lax.axis_index("dev")
    width = hot_cache.shape[1]
    hot_count = hot_cache.shape[0]
    slots = hot_count + evict_cache.shape[0]
    columns = cross_b.shape[1]

    place = me.astype(jnp.int32).reshape(1)
    masks = [int(mask) for mask in relative_masks(n)]
    groups = bit_groups(n)
    if columns % 16 == 0 and bag.shape[0] % 128 == 0:
        two, four, six = step_two, step_four, step_six
    else:
        two, four, six = plain_two, plain_four, plain_six

    w_own = cross_w.transpose(0, 2, 1)
    w1_outer = gather_outer(w_own[1].astype(bf16), n)
    w1_parts = gather_near(w1_outer, n)
    w0_outer = gather_outer(after(w_own[0].astype(bf16), w1_outer), n)
    w0_parts = gather_near(after(w0_outer, *w1_parts[: len(w1_parts) // 2]), n)

    ids = hot_slots.reshape(n, -1)
    per = ids.shape[1]
    biases_own = cross_b.astype(bf16).astype(f32).reshape(1, -1)
    first = exchange(
        after(
            jnp.concatenate(
                [ids.astype(f32), jnp.broadcast_to(biases_own, (n, 2 * columns))], axis=1
            ),
            w1_outer,
        ),
    )
    arrived_ids = first[:, :per].astype(jnp.int32)
    biases = first[:, per:].reshape(n, 2, columns).transpose(1, 0, 2).reshape(2, -1)

    slot_values = jnp.concatenate([hot_cache, evict_cache], axis=0)
    feat = pick(place, bag.T, slot_values)

    def near_sum(keep, send):
        total, _ = sum_stage(keep, [send], groups[0], n)
        return parts_of(total, groups[1])

    def own_sum(total):
        for group in groups[2:]:
            keep, parts = parts_of(total, group)
            total, _ = sum_stage(keep, parts, group, n)
        return total[0]

    feat = after(feat, w0_outer)
    bias_one, keep0, send0 = two(place, masks, w1_parts, upstream, feat)
    keep0, parts0 = near_sum(keep0, send0)
    packing = Packing(n, per, evict_dest.shape[2], columns)
    packed, keep1, send1 = four(
        place,
        masks,
        w0_parts,
        w1_parts,
        upstream,
        feat,
        biases,
        bag.T,
        slots,
        bias_one,
        packing,
        parts0,
    )
    total0, arrived0 = sum_stage(keep0, parts0, groups[1], n)
    grad0 = own_sum(total0)
    w_new0, _ = adagrad(w_own[0], cross_accum.transpose(0, 2, 1)[0], grad0, weight_rate)
    w_next = w_new0.astype(bf16)
    wn_outer = gather_outer(w_next, n)
    wn_parts = gather_near(wn_outer, n)

    keep1, parts1 = near_sum(keep1, send1)
    total1, _ = sum_stage(keep1, after(parts1, *arrived0), groups[1], n)
    grad1 = own_sum(after(total1, wn_outer))
    w_new1, _ = adagrad(w_own[1], cross_accum.transpose(0, 2, 1)[1], grad1, weight_rate)

    arrived = exchange(packed.reshape(n, -1, width)).reshape(-1, width)
    local_rows = packing.rows(arrived_ids - me * hot_table.shape[0], 0)
    bias_lanes = jnp.pad(cross_b.reshape(1, -1), ((0, 0), (0, width - 2 * columns)))
    hot_new, hot_accum_new, returned, bias_new = hot_update(
        place, local_rows, arrived, hot_table, hot_accum, bias_lanes, packing
    )
    cross_b_new = bias_new[:, : 2 * columns].reshape(2, columns)
    back = exchange(returned.reshape(n, -1, width)).reshape(-1, width)
    owner_new, owner_accum_new = owner_update(
        place, packing.rows(evict_dest[0], per), arrived, owner_table, owner_accum
    )

    next_rows = (next_bag // per) * packing.each + next_bag % per
    next_feat, next_bias = pick_next(place, next_rows.T, back, packing, feat.shape[1])
    next_first = six(place, masks, wn_parts, next_feat, next_bias)
    cross_w_new = jnp.stack([w_new0, w_new1]).transpose(0, 2, 1)
    return (
        next_first,
        hot_new,
        hot_accum_new,
        owner_new,
        owner_accum_new,
        cross_w_new,
        cross_b_new,
    )


def solution(mesh):
    return jax.shard_map(
        local,
        mesh=mesh,
        in_specs=(
            P("dev", None),
            P("dev", None),
            P("dev", None),
            P("dev"),
            P("dev", None, None),
            P("dev", None),
            P("dev", None),
            P("dev", None),
            P("dev", None),
            P("dev", None),
            P("dev", None),
            P(None, None, "dev"),
            P(None, "dev"),
            P(None, None, "dev"),
        ),
        out_specs=(
            P("dev", None),
            P("dev", None),
            P("dev", None),
            P("dev", None),
            P("dev", None),
            P(None, None, "dev"),
            P(None, "dev"),
        ),
        check_vma=False,
    )
```

```python
import math

import jax
import jax.numpy as jnp
import numpy as np
from jax import lax
from jax.experimental import pallas as pl
from jax.experimental.pallas import tpu as pltpu
from jax.sharding import PartitionSpec as P


row_rate = 0.05
weight_rate = 0.005
bias_rate = 0.0002
epsilon = 1e-10
f32 = jnp.float32
bf16 = jnp.bfloat16


def adagrad(params, accumulator, gradient, step_rate):
    updated = accumulator + gradient * gradient
    return (params - step_rate * gradient / (jnp.sqrt(updated) + epsilon), updated)


def bit_groups(devices):
    bits = devices.bit_length() - 1
    assert devices == 1 << bits
    return [(0, 1)] + [(low, min(2, bits - low)) for low in range(1, bits, 2)]


def group_masks(group):
    low, width = group
    return [value << low for value in range(1 << width)]


def relative_masks(devices):
    masks = [0]
    for group in reversed(bit_groups(devices)):
        masks = [own | inner for own in group_masks(group) for inner in masks]
    return np.array(masks, np.int32)


def swap(values, mask, devices):
    return lax.ppermute(values, "dev", [(i, i ^ mask) for i in range(devices)])


def after(values, *others):
    return lax.optimization_barrier((values, others))[0]


def gather_outer(block, devices):
    stack = block[None]
    for group in reversed(bit_groups(devices)[2:]):
        parts = [stack] + [swap(stack, mask, devices) for mask in group_masks(group)[1:]]
        stack = jnp.concatenate(parts, axis=0)
    return stack


def gather_near(stack, devices):
    masks = group_masks(bit_groups(devices)[1])[1:]
    near = [stack] + [swap(stack, mask, devices) for mask in masks]
    return near + [swap(part, 1, devices) for part in near]


def sum_stage(keep, parts, group, devices):
    total = keep.astype(f32)
    arrived = [swap(part, mask, devices) for part, mask in zip(parts, group_masks(group)[1:])]
    for part in arrived:
        total = total + part.astype(f32)
    return total, arrived


def parts_of(stack, group):
    parts = stack.reshape(len(group_masks(group)), -1, *stack.shape[1:])
    return parts[0], [parts[k].astype(bf16) for k in range(1, parts.shape[0])]


def to_absolute(parts, my_index, devices):
    stack = jnp.concatenate(parts, axis=0)
    place = np.argsort(relative_masks(devices)).astype(np.int32)
    order = jnp.asarray(place)[jnp.arange(devices, dtype=jnp.int32) ^ my_index]
    return jnp.take(stack, order, axis=0, mode="clip").reshape(-1, stack.shape[-1])


def to_relative(blocks, my_index, devices):
    order = jnp.asarray(relative_masks(devices)) ^ my_index
    return jnp.take(blocks, order, axis=0, mode="clip")


def dot(a, b, ca, cb):
    return lax.dot_general(a, b, (((ca,), (cb,)), ((), ())), preferred_element_type=f32)


def exchange(values):
    return lax.all_to_all(values, "dev", split_axis=0, concat_axis=0, tiled=True)


def one_hot(index_row, rows):
    samples = index_row.shape[1]
    return (index_row == lax.broadcasted_iota(jnp.int32, (rows, samples), 0)).astype(bf16)


def high_low(table):
    high = table.astype(bf16)
    return jnp.concatenate([high, (table - high.astype(f32)).astype(bf16)], axis=1)


def call(body, outs, inputs, scratch=(), loose=()):
    vmem = pl.BlockSpec(memory_space=pltpu.VMEM)
    count = len(inputs)

    def kernel(*refs):
        body(*refs[:count], *refs[count + len(loose) :])

    return pl.pallas_call(
        kernel,
        out_shape=[jax.ShapeDtypeStruct(*out) for out in outs],
        in_specs=[pl.BlockSpec(memory_space=pltpu.SMEM)]
        + [vmem] * (count - 1)
        + [pl.BlockSpec(memory_space=pl.ANY)] * len(loose),
        out_specs=[vmem] * len(outs),
        scratch_shapes=[pltpu.VMEM(*shape) for shape in scratch],
    )(*inputs, *loose)


def put_parts(parts, target, my_index, masks):
    place = 0
    for part in parts:
        for k in range(part.shape[0]):
            target[masks[place] ^ my_index] = part[k]
            place += 1


def give_halves(blocks, keep, send, my_index, masks):
    half = len(masks) // 2
    for place in range(half):
        keep[place] = blocks[masks[place] ^ my_index]
        send[place] = blocks[masks[half + place] ^ my_index].astype(bf16)


def chunks(rows):
    step = math.gcd(rows, 256)
    return [slice(at, at + step) for at in range(0, rows, step)]


def pick(me, index, shared, evicted):
    fields, samples = index.shape
    width = shared.shape[1]
    rows = shared.shape[0] + evicted.shape[0]

    def body(me_ref, index_ref, shared_ref, evicted_ref, out):
        both = jnp.concatenate([high_low(shared_ref[...]), high_low(evicted_ref[...])], axis=0)
        for k in range(fields):
            picked = dot(one_hot(index_ref[k : k + 1, :], rows), both, 0, 0)
            out[:, k * width : (k + 1) * width] = halves_sum(picked, width)

    return call(body, [((samples, fields * width), f32)], [me, index, shared, evicted])[0]


def pass_on(me, values):
    def body(me_ref, values_ref, out):
        out[...] = values_ref[...]

    return call(body, [(values.shape, f32)], [me, values])[0]


def step_two(me, masks, parts, upstream, feat):
    n, r, depth = len(masks), parts[0].shape[1], feat.shape[1]
    samples = feat.shape[0]

    def body(me_ref, up, feat_ref, *refs):
        refs = list(refs)
        part_refs, refs = refs[: len(parts)], refs[len(parts) :]
        bias, keep, send, w1, one_bf, feat_bf, grads = refs
        mine = me_ref[0]
        put_parts(part_refs, w1, mine, masks)
        weights = w1[...].reshape(n * r, depth)
        total = jnp.zeros((1, depth), f32)
        for at in chunks(samples):
            g = up[at].astype(f32)
            f = feat_ref[at]
            feat_bf[at] = f.astype(bf16)
            grad_layer = g + dot((g * f).astype(bf16), weights, 1, 0)
            grad_one = grad_layer * f
            total = total + jnp.sum(grad_one, axis=0, keepdims=True)
            one_bf[at] = grad_one.astype(bf16)
        bias[...] = total
        grads[...] = dot(one_bf[...], feat_bf[...], 0, 0).reshape(n, r, depth)
        give_halves(grads, keep, send, mine, masks)

    return call(
        body,
        [
            ((1, depth), f32),
            ((n // 2, r, depth), f32),
            ((n // 2, r, depth), bf16),
        ],
        [me, upstream, feat, *parts],
        [
            ((n, r, depth), bf16),
            ((samples, depth), bf16),
            ((samples, depth), bf16),
            ((n, r, depth), f32),
        ],
    )


def iota(shape, dim):
    return lax.broadcasted_iota(jnp.int32, shape, dim)


def log2(count):
    assert count & (count - 1) == 0
    return count.bit_length() - 1


class Packing:
    def __init__(self, devices, shared, evicted, columns):
        self.devices, self.shared, self.evicted = devices, shared, evicted
        self.columns = columns
        self.bias_row = shared + evicted
        self.each = 8 << max(0, (self.bias_row // 8).bit_length())
        self.total = devices * self.each

    def pack(self, slot_sum, biases):
        width = slot_sum.shape[1]
        shape = (self.total, slot_sum.shape[0])
        device, row = iota(shape, 0) >> log2(self.each), iota(shape, 0) & (self.each - 1)
        evict = self.devices * self.shared + device * self.evicted + row - self.shared
        slot = jnp.where(row < self.shared, device * self.shared + row, evict)
        slot = jnp.where(row < self.bias_row, slot, -1)
        chosen = (slot == iota(shape, 1)).astype(bf16)
        packed = halves_sum(dot(chosen, high_low(slot_sum), 1, 0), width)
        spread = jnp.zeros((self.devices, width), f32)
        for layer, bias in enumerate(biases):
            depth = bias.shape[1]
            shape = (self.devices, depth)
            own = jnp.where(iota(shape, 1) >> log2(self.columns) == iota(shape, 0), bias, 0.0)
            shape = (depth, width)
            lane = (iota(shape, 0) & (self.columns - 1)) + layer * self.columns
            to = (lane == iota(shape, 1)).astype(bf16)
            high = own.astype(bf16)
            low = (own - high.astype(f32)).astype(bf16)
            spread = spread + dot(high, to, 1, 0) + dot(low, to, 1, 0)
        shape = (self.total, self.devices)
        here = iota(shape, 0) == (iota(shape, 1) << log2(self.each)) + self.bias_row
        return packed + halves_sum(dot(here.astype(bf16), high_low(spread), 1, 0), width)

    def rows(self, values, at):
        count = values.shape[1]
        shape = (count, self.total)
        row = (iota(shape, 1) & (self.each - 1)) - at
        to = (row == iota(shape, 0)).astype(bf16)
        high = values.astype(bf16)
        low = (values - high.astype(f32)).astype(bf16)
        spread = dot(high, to, 1, 0) + dot(low, to, 1, 0)
        shape = (self.devices, self.total)
        here = iota(shape, 1) >> log2(self.each) == iota(shape, 0)
        flat = jnp.sum(jnp.where(here, spread, 0.0), axis=0, keepdims=True)
        row = (iota((1, self.total), 1) & (self.each - 1)) - at
        return jnp.where((row >= 0) & (row < count), flat.astype(jnp.int32), -1)

    def biases(self, first, depth):
        starts = (self.shared, self.shared + self.columns)
        return [self.side_by_side(first, start, depth, 1, 0) for start in starts]

    def side_by_side(self, values, first, depth, step, at):
        shape = (values.shape[1], depth)
        lane = (iota(shape, 1) & (self.columns - 1)) + first
        spread = dot(values.astype(bf16), (lane == iota(shape, 0)).astype(bf16), 1, 0)
        shape = (values.shape[0], depth)
        here = iota(shape, 0) == (iota(shape, 1) >> log2(self.columns)) * step + at
        return jnp.sum(jnp.where(here, spread, 0.0), axis=0, keepdims=True)


def step_four(me, masks, parts, parts1, upstream, feat, biases, index, slots, bias1, packing, loose):
    n, r, depth = len(masks), parts[0].shape[1], feat.shape[1]
    samples, fields = feat.shape[0], index.shape[0]
    width = depth // fields

    def body(me_ref, up, feat_ref, biases_ref, index_ref, bias1_ref, *refs):
        refs = list(refs)
        count = len(parts)
        packed, keep, send, w0, w1, layer_bf, two_bf, feat_grad, grads = refs[2 * count :]
        mine = me_ref[0]
        put_parts(refs[:count], w0, mine, masks)
        put_parts(refs[count : 2 * count], w1, mine, masks)
        first = w0[...].reshape(n * r, depth)
        second = w1[...].reshape(n * r, depth)
        total = jnp.zeros((1, depth), f32)
        bias = packing.biases(biases_ref[...], depth)
        for at in chunks(samples):
            g = up[at].astype(f32)
            f = feat_ref[at]
            two = g * f
            total = total + jnp.sum(two, axis=0, keepdims=True)
            two_bf[at] = two.astype(bf16)
            proj_one = dot(f.astype(bf16), first, 1, 1) + bias[0]
            layer_bf[at] = (f * proj_one + f).astype(bf16)
            proj_two = dot(layer_bf[at], second, 1, 1) + bias[1]
            layer = g + dot(two_bf[at], second, 1, 0)
            grad_feat = g * proj_two + layer * (proj_one + 1.0)
            grad_feat = grad_feat + dot((layer * f).astype(bf16), first, 1, 0)
            feat_grad[at] = grad_feat.astype(bf16)
        slot_sum = jnp.zeros((slots, width), f32)
        for k in range(fields):
            block = feat_grad[:, k * width : (k + 1) * width]
            slot_sum = slot_sum + dot(one_hot(index_ref[k : k + 1, :], slots), block, 1, 0)
        packed[...] = packing.pack(slot_sum, (bias1_ref[...], total))
        grads[...] = dot(two_bf[...], layer_bf[...], 0, 0).reshape(n, r, depth)
        give_halves(grads, keep, send, mine, masks)

    return call(
        body,
        [
            ((packing.total, width), f32),
            ((n // 2, r, depth), f32),
            ((n // 2, r, depth), bf16),
        ],
        [me, upstream, feat, biases, index, bias1, *parts, *parts1],
        [
            ((n, r, depth), bf16),
            ((n, r, depth), bf16),
            ((samples, depth), bf16),
            ((samples, depth), bf16),
            ((samples, depth), bf16),
            ((n, r, depth), f32),
        ],
        loose,
    )


def pick_next(index, values, packing):
    width = values.shape[1]
    rows = ((index >> log2(packing.shared)) << log2(packing.each)) + (
        index & (packing.shared - 1)
    )
    both = high_low(values)
    for k in range(index.shape[0]):
        yield halves_sum(dot(one_hot(rows[k : k + 1], values.shape[0]), both, 0, 0), width)


def step_six(me, masks, parts, index, back, packing):
    n, r, depth = len(masks), parts[0].shape[1], parts[0].shape[2]
    samples, width = index.shape[1], back.shape[1]

    def body(me_ref, index_ref, back_ref, *refs):
        part_refs, (out, wn, feat_ref) = refs[: len(parts)], refs[len(parts) :]
        put_parts(part_refs, wn, me_ref[0], masks)
        weights = wn[...].reshape(n * r, depth)
        values = back_ref[...]
        for k, picked in enumerate(pick_next(index_ref[...], values, packing)):
            feat_ref[:, k * width : (k + 1) * width] = picked
        bias = packing.side_by_side(values, 0, depth, packing.each, packing.bias_row)
        for at in chunks(samples):
            f = feat_ref[at]
            proj = dot(f.astype(bf16), weights, 1, 1) + bias
            out[at] = (f * proj + f).astype(bf16)

    return call(
        body,
        [((samples, depth), bf16)],
        [me, index, back, *parts],
        [((n, r, depth), bf16), ((samples, depth), f32)],
    )[0]


def halves_sum(both, width):
    return both[:, :width] + both[:, width:]


def hot_update(me, first, arrived, table, accum, bias, packing):
    width = table.shape[1]

    def body(me_ref, first_ref, arrived_ref, table_ref, accum_ref, bias_ref, *outs):
        new, accum_new, returned, bias_new = outs
        values = arrived_ref[...]
        place = iota(values.shape, 0) & (packing.each - 1)
        bias_sum = jnp.where(place == packing.bias_row, values, 0.0)
        bias_sum = jnp.sum(bias_sum, axis=0, keepdims=True)
        stepped = bias_ref[...] - bias_rate * bias_sum
        bias_new[...] = stepped
        rows = packing.rows(first_ref[:, : packing.shared], 0)
        rows = jnp.where(rows < 0, -1, rows - me_ref[0] * table.shape[0])
        chosen = one_hot(rows, table.shape[0])
        gradient = halves_sum(dot(chosen, high_low(values), 1, 0), width)
        updated, accum_new[...] = adagrad(table_ref[...], accum_ref[...], gradient, row_rate)
        new[...] = updated
        back = halves_sum(dot(chosen, high_low(updated), 0, 0), width)
        returned[...] = jnp.where(
            place == packing.bias_row, stepped.astype(bf16).astype(f32), back
        )

    return call(
        body,
        [(table.shape, f32), (table.shape, f32), (arrived.shape, f32), ((1, width), f32)],
        [me, first, arrived, table, accum, bias],
    )


def owner_update(me, targets, moved, table, accum, packing):
    width = table.shape[1]

    def body(me_ref, targets_ref, moved_ref, table_ref, accum_ref, new, accum_new):
        rows = packing.rows(targets_ref[...], packing.shared)
        chosen = one_hot(rows, table.shape[0])
        gradient = halves_sum(dot(chosen, high_low(moved_ref[...]), 1, 0), width)
        new[...], accum_new[...] = adagrad(table_ref[...], accum_ref[...], gradient, row_rate)

    return call(body, [(table.shape, f32), (table.shape, f32)], [me, targets, moved, table, accum])


def plain_halves(grads, me, masks):
    n = len(masks)
    placed = to_relative(grads.reshape(n, -1, grads.shape[1]), me[0], n)
    return placed[: n // 2], placed[n // 2 :].astype(bf16)


def plain_two(me, masks, parts, upstream, feat):
    w1 = to_absolute(parts, me[0], len(masks))
    g = upstream.astype(f32)
    layer = g + dot((g * feat).astype(bf16), w1, 1, 0)
    grad_one = layer * feat
    one_bf = grad_one.astype(bf16)
    keep, send = plain_halves(dot(one_bf, feat.astype(bf16), 0, 0), me, masks)
    return jnp.sum(grad_one, axis=0, keepdims=True), keep, send


def plain_four(me, masks, parts, parts1, upstream, feat, biases, index, slots, bias1, packing, loose):
    w0 = to_absolute(parts, me[0], len(masks))
    w1 = to_absolute(parts1, me[0], len(masks))
    bias = packing.biases(biases, feat.shape[1])
    g = upstream.astype(f32)
    two = g * feat
    proj_one = dot(feat.astype(bf16), w0, 1, 1) + bias[0]
    layer_bf = (feat * proj_one + feat).astype(bf16)
    proj_two = dot(layer_bf, w1, 1, 1) + bias[1]
    layer = g + dot(two.astype(bf16), w1, 1, 0)
    one_bf = (layer * feat).astype(bf16)
    grad_feat = g * proj_two + layer * (proj_one + 1.0) + dot(one_bf, w0, 1, 0)
    grad_feat = grad_feat.astype(bf16)
    width = feat.shape[1] // index.shape[0]
    slot = sum(
        dot(one_hot(row[None], slots), grad_feat[:, k * width : (k + 1) * width], 1, 0)
        for k, row in enumerate(index)
    )
    keep, send = plain_halves(dot(two.astype(bf16), layer_bf, 0, 0), me, masks)
    packed = packing.pack(slot, (bias1, jnp.sum(two, axis=0, keepdims=True)))
    return packed, keep, send


def plain_six(me, masks, parts, index, back, packing):
    wn = to_absolute(parts, me[0], len(masks))
    feat = jnp.concatenate(list(pick_next(index, back, packing)), axis=1)
    bias = packing.side_by_side(back, 0, wn.shape[1], packing.each, packing.bias_row)
    proj = dot(feat.astype(bf16), wn, 1, 1) + bias
    return (feat * proj + feat).astype(bf16)


def local(
    upstream,
    bag,
    next_bag,
    hot_slots,
    evict_dest,
    hot_cache,
    evict_cache,
    hot_table,
    hot_accum,
    owner_table,
    owner_accum,
    cross_w,
    cross_b,
    cross_accum,
):
    n = lax.axis_size("dev")
    me = lax.axis_index("dev")
    width = hot_cache.shape[1]
    hot_count = hot_cache.shape[0]
    slots = hot_count + evict_cache.shape[0]
    columns = cross_b.shape[1]

    place = me.astype(jnp.int32).reshape(1)
    masks = [int(mask) for mask in relative_masks(n)]
    groups = bit_groups(n)
    if columns % 16 == 0 and bag.shape[0] % 128 == 0:
        two, four, six = step_two, step_four, step_six
    else:
        two, four, six = plain_two, plain_four, plain_six

    w_own = cross_w.transpose(0, 2, 1)
    w1_outer = gather_outer(w_own[1].astype(bf16), n)
    w1_parts = gather_near(w1_outer, n)
    w0_outer = gather_outer(after(w_own[0].astype(bf16), w1_outer), n)
    w0_parts = gather_near(after(w0_outer, *w1_parts[: len(w1_parts) // 2]), n)

    ids = hot_slots.reshape(n, -1)
    per = ids.shape[1]
    biases_own = cross_b.astype(bf16).astype(f32).reshape(1, -1)
    first = exchange(
        after(
            jnp.concatenate(
                [ids.astype(f32), jnp.broadcast_to(biases_own, (n, 2 * columns))], axis=1
            ),
            w1_outer,
        ),
    )
    packing = Packing(n, per, evict_dest.shape[2], columns)
    bias_lanes = jnp.pad(cross_b.reshape(1, -1), ((0, 0), (0, width - 2 * columns)))
    bias_lanes = pass_on(place, bias_lanes)

    feat = pick(place, bag.T, hot_cache, evict_cache)

    def near_sum(keep, send):
        total, _ = sum_stage(keep, [send], groups[0], n)
        return parts_of(total, groups[1])

    def own_sum(total):
        for group in groups[2:]:
            keep, parts = parts_of(total, group)
            total, _ = sum_stage(keep, parts, group, n)
        return total[0]

    feat = after(feat, w0_outer)
    bias_one, keep0, send0 = two(place, masks, w1_parts, upstream, feat)
    keep0, parts0 = near_sum(keep0, send0)
    packed, keep1, send1 = four(
        place,
        masks,
        w0_parts,
        w1_parts,
        upstream,
        feat,
        first,
        bag.T,
        slots,
        bias_one,
        packing,
        parts0,
    )
    total0, arrived0 = sum_stage(keep0, parts0, groups[1], n)
    grad0 = own_sum(total0)
    w_new0, _ = adagrad(w_own[0], cross_accum.transpose(0, 2, 1)[0], grad0, weight_rate)
    w_next = w_new0.astype(bf16)
    wn_outer = gather_outer(w_next, n)
    wn_parts = gather_near(wn_outer, n)

    keep1, parts1 = near_sum(keep1, send1)
    total1, _ = sum_stage(keep1, after(parts1, *arrived0), groups[1], n)
    grad1 = own_sum(after(total1, wn_outer))
    w_new1, _ = adagrad(w_own[1], cross_accum.transpose(0, 2, 1)[1], grad1, weight_rate)

    arrived = exchange(packed.reshape(n, -1, width)).reshape(-1, width)
    hot_new, hot_accum_new, returned, bias_new = hot_update(
        place, first, arrived, hot_table, hot_accum, bias_lanes, packing
    )
    cross_b_new = bias_new[:, : 2 * columns].reshape(2, columns)
    back = exchange(returned.reshape(n, -1, width)).reshape(-1, width)
    owner_new, owner_accum_new = owner_update(
        place, evict_dest[0].astype(f32), arrived, owner_table, owner_accum, packing
    )

    next_first = six(place, masks, wn_parts, next_bag.T, back, packing)
    cross_w_new = jnp.stack([w_new0, w_new1]).transpose(0, 2, 1)
    return (
        next_first,
        hot_new,
        hot_accum_new,
        owner_new,
        owner_accum_new,
        cross_w_new,
        cross_b_new,
    )


def solution(mesh):
    return jax.shard_map(
        local,
        mesh=mesh,
        in_specs=(
            P("dev", None),
            P("dev", None),
            P("dev", None),
            P("dev"),
            P("dev", None, None),
            P("dev", None),
            P("dev", None),
            P("dev", None),
            P("dev", None),
            P("dev", None),
            P("dev", None),
            P(None, None, "dev"),
            P(None, "dev"),
            P(None, None, "dev"),
        ),
        out_specs=(
            P("dev", None),
            P("dev", None),
            P("dev", None),
            P("dev", None),
            P("dev", None),
            P(None, None, "dev"),
            P(None, "dev"),
        ),
        check_vma=False,
    )
```
